32 devices in a mesh: row: 8 (over y, x, core), col: 4 (over z).
Axes of the slice: x: 2, y: 2, z: 4, core: 2. Of those that a mesh axis runs over, the one named last changes fastest.
Arguments:
- query: bfloat16 [8, 512, 4096], P(None, 'col'), may hold values from -7 to 7
- key: bfloat16 [4096, 512], P(('row', 'col')), may hold values from -7 to 7
- value: bfloat16 [4096, 512], P(('row', 'col')), may hold values from -4 to 4
- span_order: int32 [32], replicated, may hold values from 0 to 31, each once
Outputs:
- attention: bfloat16 [4096, 4096], P(('row', 'col'))
The draws below stay inside these ranges and needn't reach their ends.
Inputs may be any that keep to these rules, and one draw needn't show every extreme that they name: span_order is a permutation of 0 to 31.
All inputs are finite; a program needn't handle non-finite values.
Results may differ from the reference program's by a relative error of at most 0.0085.
Values may be sent and summed in bfloat16 or wider, within the bound.
A program may use at most 192 MiB of HBM per device.

```python
import jax
import jax.numpy as jnp
from jax import lax

HEAD_DIM = 128
QHEADS = 32
KVHEADS = 4
TOK_DEV = 128
GROUP_ROWS = 512
SPANS = 32
SEQ = 4096


def draw_pair(key):
    first = jax.random.fold_in(key, 101)
    second = jax.random.fold_in(key, 202)
    key_part = jnp.clip(1.75 * jax.random.normal(first, (SEQ, KVHEADS * HEAD_DIM), jnp.float32), -7.0, 7.0)
    query_part = jnp.clip(1.75 * jax.random.normal(second, (SEQ, QHEADS * HEAD_DIM), jnp.float32), -7.0, 7.0)
    return (query_part, key_part)


def draw_query(key, part):
    query_part, unused = draw_pair(key)
    return query_part.reshape(SEQ // GROUP_ROWS, GROUP_ROWS, QHEADS * HEAD_DIM).astype(jnp.bfloat16)


def draw_key(key, part):
    unused, key_part = draw_pair(key)
    return key_part.astype(jnp.bfloat16)


def shard_levels(stream_key, extent, pieces, smallest, high):
    def one(dim, parts):
        draws = jax.random.uniform(jax.random.fold_in(jax.random.fold_in(stream_key, 6), dim), (parts,), jnp.float32, smallest / len(pieces), high / len(pieces))
        return jnp.repeat(jnp.exp(draws), extent[dim] // parts).reshape((-1,) + (1,) * (len(extent) - dim - 1))

    level = one(*pieces[0])
    for cut in pieces[1:]:
        level = level * one(*cut)
    return level


def scatter_about(rng, dims, scale, bound, shards=(), kind=jnp.bfloat16):
    factor_of = shard_levels(rng, dims, shards, -0.22, 0.18) if shards else 1.0
    array = jax.random.normal(rng, dims, jnp.float32) * scale * factor_of
    return jnp.minimum(jnp.maximum(array, -bound), bound).astype(kind)


def setup_inputs(seed: int = 0) -> dict:
    seeds = jax.random.split(jax.random.key(seed), 5)
    query = draw_query(jax.random.fold_in(seeds[4], 71), 0)
    key = draw_key(jax.random.fold_in(seeds[4], 71), 0)
    value = scatter_about(seeds[2], (SEQ, KVHEADS * HEAD_DIM), 1.0, 4.0, ((0, 32),))
    span_order = jax.random.permutation(seeds[3], SPANS).astype(jnp.int32)
    return dict(query=query, key=key, value=value, span_order=span_order)


masked_score = -1.0e30


def reference(query, key, value, span_order):
    group = QHEADS // KVHEADS
    groups = SEQ // GROUP_ROWS
    offsets = jnp.arange(TOK_DEV, dtype=jnp.int32)
    positions = (span_order.astype(jnp.int32)[:, None] * TOK_DEV + offsets[None, :]).astype(jnp.int32)
    queries = query.reshape(SPANS, TOK_DEV, KVHEADS, group, HEAD_DIM)
    keys = key.reshape(groups, GROUP_ROWS, KVHEADS, HEAD_DIM)
    values = value.reshape(groups, GROUP_ROWS, KVHEADS, HEAD_DIM)
    key_places = positions.reshape(groups, GROUP_ROWS)

    def one_span(inputs):
        span_queries, span_places = inputs
        span_queries = span_queries.astype(jnp.float32)

        def live_group(group_in):
            group_keys, group_values, group_places = group_in
            scores = jnp.einsum("nkgd,skd->nkgs", span_queries, group_keys.astype(jnp.float32)) * (HEAD_DIM ** -0.5)
            visible = group_places[None, None, None, :] <= span_places[:, None, None, None]
            scores = jnp.where(visible, scores, masked_score)
            top = jnp.max(scores, axis=-1)
            raised = jnp.exp(scores - top[..., None])
            total = jnp.sum(raised, axis=-1)
            weights = lax.optimization_barrier(raised.astype(jnp.bfloat16)).astype(jnp.float32)
            summed = jnp.einsum("nkgs,skd->nkgd", weights, group_values.astype(jnp.float32))
            floor = jnp.maximum(total, 1.0)
            partial_value = lax.optimization_barrier((summed / floor[..., None]).astype(jnp.bfloat16)).astype(jnp.float32)
            return partial_value, top + jnp.log(floor)

        def dead_group(group_in):
            partial_value = jnp.zeros((TOK_DEV, KVHEADS, group, HEAD_DIM), span_queries.dtype)
            log_sum = jnp.full((TOK_DEV, KVHEADS, group), masked_score, span_queries.dtype)
            return partial_value, log_sum

        def one_group(group_in):
            group_places = group_in[2]
            alive = jnp.min(group_places) <= jnp.max(span_places)
            return lax.cond(alive, live_group, dead_group, group_in)

        partials, log_sums = lax.map(one_group, (keys, values, key_places))
        highest = jnp.max(log_sums, axis=0)
        combined = highest + jnp.log(jnp.sum(jnp.exp(log_sums - highest), axis=0))
        scale_each = jnp.exp(log_sums - combined)
        merged = jnp.sum(scale_each[..., None] * partials, axis=0)
        return merged.astype(jnp.bfloat16)

    result = lax.map(one_span, (queries, positions))
    return result.reshape(SEQ, QHEADS * HEAD_DIM)
```

```python
import functools
import math

import jax
import jax.numpy as jnp
from jax import lax
from jax.experimental import pallas as pl
from jax.experimental.pallas import tpu as pltpu
from jax.sharding import PartitionSpec as P

HEAD_DIM = 128
KVHEADS = 4
SIDE = 2
masked_score = -1e30
MESH = pl.DeviceIdType.MESH
VMEM_LIMIT = 60 * 1024 * 1024
ONES = 16
SCALE = math.log2(math.e) / math.sqrt(HEAD_DIM)


def device(row, col):
    return {"row": row, "col": col}


def fused_kernel(rows, cols, heads, order_hbm, query_hbm, key_hbm, value_hbm, out_ref,
                 order_ref, query_ref, key_ref, value_ref, turned, held, queries, scores_even, scores_odd,
                 total, best, tops, lower, stage,
                 load_sem, plane_send, plane_recv, col_send, col_recv, side_send, side_recv,
                 own_sem, part_send, part_recv):
    share = rows // KVHEADS
    tokens = key_ref.shape[0]
    width = heads * tokens
    block = 2 * tokens
    blocks = rows * tokens // block
    units = rows * cols
    row, col = lax.axis_index("row"), lax.axis_index("col")
    head, lane = row // share, row % share
    ways = (1, -1)

    here = pl.ds(pl.multiple_of(head * HEAD_DIM, HEAD_DIM), HEAD_DIM)
    mine = pl.ds(pl.multiple_of(row * width, width), width)
    loads = [
        pltpu.make_async_copy(value_hbm, value_ref, load_sem.at[0]),
        pltpu.make_async_copy(key_hbm, key_ref, load_sem.at[1]),
        pltpu.make_async_copy(key_hbm.at[:, here], held.at[col, row, 0], load_sem.at[2]),
        pltpu.make_async_copy(order_hbm, order_ref, load_sem.at[3]),
        pltpu.make_async_copy(query_hbm.at[:, :, mine], query_ref, load_sem.at[4]),
    ]
    for load in loads:
        load.start()

    barrier = pltpu.get_barrier_semaphore()
    for step in range(1, rows):
        pl.semaphore_signal(
            barrier, inc=1, device_id=device(lax.rem(row + step, rows), col), device_id_type=MESH
        )
    for way in ways:
        @pl.when(jnp.logical_and(col + way >= 0, col + way < cols))
        def _(way=way):
            pl.semaphore_signal(barrier, inc=1, device_id=device(row, col + way), device_id_type=MESH)

    ends = jnp.where(col == 0, 1, 0) + jnp.where(col == cols - 1, 1, 0)

    def chip_at(step):
        along = lax.rem(head % SIDE + step % SIDE, SIDE)
        return lax.rem(head // SIDE + step // SIDE, SIDE) * SIDE + along

    loads[0].wait()
    for other in range(KVHEADS):
        turned[other] = value_ref[:, other * HEAD_DIM : (other + 1) * HEAD_DIM].T
    held[col, row, 1] = turned[head]
    loads[1].wait()
    loads[2].wait()
    pl.semaphore_wait(barrier, rows - 1 + len(ways) - ends)

    plane = []
    for step in range(1, KVHEADS):
        other = chip_at(step)
        columns = pl.ds(pl.multiple_of(other * HEAD_DIM, HEAD_DIM), HEAD_DIM)
        for kind, source in enumerate((key_ref.at[:, columns], turned.at[other])):
            copy = pltpu.make_async_remote_copy(
                src_ref=source,
                dst_ref=held.at[col, row, kind],
                send_sem=plane_send.at[step - 1, kind],
                recv_sem=plane_recv.at[step - 1, kind],
                device_id=device(other * share + lane, col),
                device_id_type=MESH,
            )
            copy.start()
            plane.append(copy)

    def plane_in(piece, kind):
        spot = held.at[col, chip_at(piece) * share + lane, kind]
        return pltpu.make_async_remote_copy(
            src_ref=spot,
            dst_ref=spot,
            send_sem=plane_send.at[piece - 1, kind],
            recv_sem=plane_recv.at[piece - 1, kind],
            device_id=device(chip_at(piece) * share + lane, col),
            device_id_type=MESH,
        )

    def held_here(step, way):
        source = col - way * step
        return jnp.logical_and(source >= 0, source < cols)

    def passes_on(step, way):
        target = col + way
        return jnp.logical_and(held_here(step, way), jnp.logical_and(target >= 0, target < cols))

    def col_copy(step, way, piece, arriving):
        source = col - way * (step + 1) if arriving else col - way * step
        spot = held.at[source, chip_at(piece) * share + lane]
        return pltpu.make_async_remote_copy(
            src_ref=spot,
            dst_ref=spot,
            send_sem=col_send.at[step, ways.index(way), piece],
            recv_sem=col_recv.at[step, ways.index(way), piece],
            device_id=device(row, col - way if arriving else col + way),
            device_id_type=MESH,
        )

    def side_copy(source, piece, other, arriving):
        there = lax.rem(lane - other + share, share) if arriving else lane
        spot = held.at[source, chip_at(piece) * share + there]
        return pltpu.make_async_remote_copy(
            src_ref=spot,
            dst_ref=spot,
            send_sem=side_send.at[source, piece, other - 1],
            recv_sem=side_recv.at[source, piece, other - 1],
            device_id=device(head * share + lax.rem(lane + other, share), col),
            device_id_type=MESH,
        )

    def relay(step, piece):
        for way in ways:
            if step:
                @pl.when(held_here(step, way))
                def _(way=way):
                    col_copy(step - 1, way, piece, True).wait_recv()

            if step < cols - 1:
                @pl.when(passes_on(step, way))
                def _(way=way):
                    col_copy(step, way, piece, False).start()

            if step or way == 1:
                @pl.when(held_here(step, way))
                def _(way=way):
                    for other in range(1, share):
                        side_copy(col - way * step, piece, other, False).start()

    for piece in range(KVHEADS):
        if piece:
            plane_in(piece, 0).wait_recv()
            plane_in(piece, 1).wait_recv()
        relay(0, piece)

    loads[4].wait()
    for index in range(rows):
        for member in range(heads):
            queries[index, :, member * tokens : (member + 1) * tokens] = query_ref[
                index, :, member * HEAD_DIM : (member + 1) * HEAD_DIM
            ].T
    across = lax.broadcasted_iota(jnp.int32, (tokens, tokens), 1)
    lower[...] = lax.broadcasted_iota(jnp.int32, (tokens, tokens), 0) - across
    loads[3].wait()

    left, right = col, cols - 1 - col
    both = jnp.minimum(left, right)

    def plane_of(phase):
        near = (phase + 1) // 2
        paired = jnp.where(phase % 2 == 1, col - near, col + near)
        far = phase - both
        single = jnp.where(left > right, col - far, col + far)
        return jnp.where(phase <= 2 * both, paired, single)

    def block_of(turn):
        half = share // 2
        slot, part = turn // half, half - 1 - turn % half
        outer = 1 - slot // 6
        along = outer * (1 - (slot % 2) * (slot // 3))
        down = outer * (1 - ((slot + 1) % 2) * ((slot + 1) // 3))
        shift = jnp.where(slot < 2, slot, jnp.where(slot < 6, slot // 4, 7 - slot))
        chip = lax.rem(head // SIDE + down, SIDE) * SIDE + lax.rem(head % SIDE + along, SIDE)
        return chip * share + lax.rem(lane + shift * half + part, share)

    def ready(phase):
        source = plane_of(phase) if phase else col
        for piece in range(KVHEADS):
            for other in range(1, share):
                side_copy(source, piece, other, True).wait_recv()

    def produce(phase, turn, part, buffer, newest):
        source = plane_of(phase) if phase else col
        index = block_of(turn)
        place = order_ref[index * cols + col]
        keys = held[source, 2 * part : 2 * part + 2, 0].reshape(block, HEAD_DIM)
        scores = jnp.dot(keys, queries[index], preferred_element_type=jnp.float32)
        for half in range(2):
            span = 2 * part + half
            lines = scores[half * tokens : (half + 1) * tokens]
            if phase == 0:
                limit = jnp.where(index == span, 0, tokens)
                shown = jnp.concatenate([lower[...]] * heads, axis=1) <= limit
                lines = jnp.where(shown, lines, masked_score)
            buffer[span * tokens : (span + 1) * tokens, :] = lines
            top = jnp.max(lines.reshape(tokens // 8, 8, width), axis=0)
            newest = jnp.maximum(newest, jnp.where(order_ref[span * cols + source] <= place, top, masked_score))
        return newest

    def consume(phase, turn, part, buffer, level, summed):
        source = plane_of(phase) if phase else col
        place = order_ref[block_of(turn) * cols + col]
        raised, columns = [], []
        for half in range(2):
            span = 2 * part + half
            ceiling = jnp.where(order_ref[span * cols + source] <= place, level, -masked_score)
            lines = buffer[span * tokens : (span + 1) * tokens, :]
            raised.append(jnp.exp2(lines * SCALE - ceiling).astype(jnp.bfloat16))
            columns.append(held[source, span, 1])
        ones = jnp.ones((ONES, block), jnp.bfloat16)
        weighed = jnp.concatenate([jnp.concatenate(columns, axis=1), ones], axis=0)
        update = jnp.dot(weighed, jnp.concatenate(raised, axis=0), preferred_element_type=jnp.float32)
        return update if summed is None else summed + update

    def first(phase, turn, buffer):
        newest = jnp.full((8, width), masked_score, jnp.float32)
        for part in range(blocks):
            newest = produce(phase, turn, part, buffer, newest)
        tops[...] = newest

    def unit(phase, turn, now, later, following):
        index = block_of(turn)
        highest = jnp.max(tops[...], axis=0, keepdims=True)
        if phase:
            before = best[index, 0:1, :]
            highest = jnp.maximum(before, highest)
            shrink = jnp.exp2((before - highest) * SCALE)
        level = highest * SCALE
        best[index] = jnp.broadcast_to(highest, (8, width))
        newest = jnp.full((8, width), masked_score, jnp.float32)
        summed = None
        for part in range(blocks):
            if following is not None:
                newest = produce(*following, part, later, newest)
            summed = consume(phase, turn, part, now, level, summed)
        if following is not None:
            tops[...] = newest
        if phase:
            summed = total[index] * shrink + summed
        if phase < cols - 1:
            total[index] = summed
        else:
            share_of = summed[:HEAD_DIM] / summed[HEAD_DIM : HEAD_DIM + 1]
            for member in range(heads):
                stage[turn, :, member * HEAD_DIM : (member + 1) * HEAD_DIM] = (
                    share_of[:, member * tokens : (member + 1) * tokens].T.astype(stage.dtype)
                )

    def part_copy(turn):
        return pltpu.make_async_remote_copy(
            src_ref=stage.at[turn],
            dst_ref=out_ref.at[:, mine],
            send_sem=part_send.at[turn],
            recv_sem=part_recv.at[turn],
            device_id=device(block_of(turn), col),
            device_id_type=MESH,
        )

    pairs = rows // 2
    ready(0)
    first(0, 0, scores_even)
    for phase in range(cols):
        final = phase == cols - 1

        def body(pair, carry, phase=phase, final=final):
            turn = 2 * pair
            if not final:
                for piece in range(KVHEADS):
                    @pl.when(pair == (piece + 1) * pairs // (KVHEADS + 1))
                    def _(piece=piece):
                        relay(phase + 1, piece)
            unit(phase, turn, scores_even, scores_odd, (phase, turn + 1))
            if final:
                part_copy(turn).start()
            unit(phase, turn + 1, scores_odd, scores_even, (phase, turn + 2))
            if final:
                part_copy(turn + 1).start()
            return carry

        lax.fori_loop(0, pairs - 1, body, 0)
        turn = rows - 2
        if not final:
            for piece in range(KVHEADS):
                if (piece + 1) * pairs // (KVHEADS + 1) >= pairs - 1:
                    relay(phase + 1, piece)
        unit(phase, turn, scores_even, scores_odd, (phase, turn + 1))
        if final:
            part_copy(turn).start()
            unit(phase, turn + 1, scores_odd, scores_even, None)
        else:
            ready(phase + 1)
            unit(phase, turn + 1, scores_odd, scores_even, (phase + 1, 0))

    own = pltpu.make_async_copy(stage.at[rows - 1], out_ref.at[:, mine], own_sem)
    own.start()
    for copy in plane:
        copy.wait_send()
    for step in range(cols):
        for way in ways:
            if step < cols - 1:
                @pl.when(passes_on(step, way))
                def _(way=way):
                    for piece in range(KVHEADS):
                        col_copy(step, way, piece, False).wait_send()

            if step or way == 1:
                @pl.when(held_here(step, way))
                def _(way=way):
                    for piece in range(KVHEADS):
                        for other in range(1, share):
                            side_copy(col - way * step, piece, other, False).wait_send()
    own.wait()
    for turn in range(rows - 1):
        part_copy(turn).wait()


def fused(query, key, value, span_order, rows, cols):
    tokens = key.shape[0]
    share = rows // KVHEADS
    width = query.shape[2] // rows
    heads = width // HEAD_DIM
    lines = heads * tokens
    kind = query.dtype
    real = jnp.float32
    dma = pltpu.SemaphoreType.DMA
    return pl.pallas_call(
        functools.partial(fused_kernel, rows, cols, heads),
        out_shape=jax.ShapeDtypeStruct((tokens, rows * width), kind),
        in_specs=[pl.BlockSpec(memory_space=pl.ANY)] * 4,
        out_specs=pl.BlockSpec(memory_space=pl.ANY),
        scratch_shapes=[
            pltpu.SMEM(span_order.shape, jnp.int32),
            pltpu.VMEM((rows, tokens, width), kind),
            pltpu.VMEM(key.shape, kind),
            pltpu.VMEM(value.shape, kind),
            pltpu.VMEM((KVHEADS, HEAD_DIM, tokens), kind),
            pltpu.VMEM((cols, rows, 2, tokens, HEAD_DIM), kind),
            pltpu.VMEM((rows, HEAD_DIM, lines), kind),
            pltpu.VMEM((rows * tokens, lines), real),
            pltpu.VMEM((rows * tokens, lines), real),
            pltpu.VMEM((rows, HEAD_DIM + ONES, lines), real),
            pltpu.VMEM((rows, 8, lines), real),
            pltpu.VMEM((8, lines), real),
            pltpu.VMEM((tokens, tokens), jnp.int32),
            pltpu.VMEM((rows, tokens, width), kind),
            dma((5,)),
            dma((KVHEADS - 1, 2)),
            dma((KVHEADS - 1, 2)),
            dma((cols - 1, 2, KVHEADS)),
            dma((cols - 1, 2, KVHEADS)),
            dma((cols, KVHEADS, share - 1)),
            dma((cols, KVHEADS, share - 1)),
            dma(()),
            dma((rows - 1,)),
            dma((rows - 1,)),
        ],
        compiler_params=pltpu.CompilerParams(
            collective_id=0, has_side_effects=True, vmem_limit_bytes=VMEM_LIMIT
        ),
        name="fused",
    )(span_order, query, key, value)


def shards(query, key, value, span_order):
    return fused(query, key, value, span_order, lax.axis_size("row"), lax.axis_size("col"))


def solution(mesh):
    placed = (P(None, "col", None), P(("row", "col"), None), P(("row", "col"), None), P())
    return jax.shard_map(
        shards, mesh=mesh, in_specs=placed, out_specs=P(("row", "col"), None), check_vma=False
    )
```

```python
import functools
import math

import jax
import jax.numpy as jnp
from jax import lax
from jax.experimental import pallas as pl
from jax.experimental.pallas import tpu as pltpu
from jax.sharding import PartitionSpec as P

HEAD_DIM = 128
KVHEADS = 4
SIDE = 2
masked_score = -1e30
MESH = pl.DeviceIdType.MESH
VMEM_LIMIT = 40 * 1024 * 1024
ONES = 16
SCALE = math.log2(math.e) / math.sqrt(HEAD_DIM)
TILE = 256
POS = (0, 2, 2, 4)


def device(row, col):
    return {"row": row, "col": col}


def fused_kernel(rows, cols, heads, order_hbm, query_hbm, key_hbm, value_hbm, out_ref,
                 order_ref, query_ref, key_ref, value_ref, turned, held, queries, scores_even, scores_odd,
                 total, best, tops, lower, stage,
                 load_sem, plane_send, plane_recv, col_send, col_recv, side_send, side_recv,
                 own_sem, part_send, part_recv):
    share = rows // KVHEADS
    tokens = key_ref.shape[0]
    width = heads * tokens
    block = 2 * tokens
    tile = min(width, TILE)
    row, col = lax.axis_index("row"), lax.axis_index("col")
    head, lane = row // share, row % share
    ways = (1, -1)

    here = pl.ds(pl.multiple_of(head * HEAD_DIM, HEAD_DIM), HEAD_DIM)
    mine = pl.ds(pl.multiple_of(row * width, width), width)
    loads = [
        pltpu.make_async_copy(value_hbm, value_ref, load_sem.at[0]),
        pltpu.make_async_copy(key_hbm, key_ref, load_sem.at[1]),
        pltpu.make_async_copy(key_hbm.at[:, here], held.at[col, row, 0], load_sem.at[2]),
        pltpu.make_async_copy(order_hbm, order_ref, load_sem.at[3]),
        pltpu.make_async_copy(query_hbm.at[:, :, mine], query_ref, load_sem.at[4]),
    ]
    for load in loads:
        load.start()

    barrier = pltpu.get_barrier_semaphore()
    for step in range(1, rows):
        pl.semaphore_signal(
            barrier, inc=1, device_id=device(lax.rem(row + step, rows), col), device_id_type=MESH
        )
    for way in ways:
        @pl.when(jnp.logical_and(col + way >= 0, col + way < cols))
        def _(way=way):
            pl.semaphore_signal(barrier, inc=1, device_id=device(row, col + way), device_id_type=MESH)

    ends = jnp.where(col == 0, 1, 0) + jnp.where(col == cols - 1, 1, 0)

    def chip_at(step):
        along = lax.rem(head % SIDE + step % SIDE, SIDE)
        return lax.rem(head // SIDE + step // SIDE, SIDE) * SIDE + along

    loads[0].wait()
    for other in range(KVHEADS):
        turned[other] = value_ref[:, other * HEAD_DIM : (other + 1) * HEAD_DIM].T
    held[col, row, 1] = turned[head]
    loads[1].wait()
    loads[2].wait()
    pl.semaphore_wait(barrier, rows - 1 + len(ways) - ends)

    plane = []
    for step in range(1, KVHEADS):
        other = chip_at(step)
        columns = pl.ds(pl.multiple_of(other * HEAD_DIM, HEAD_DIM), HEAD_DIM)
        for kind, source in enumerate((key_ref.at[:, columns], turned.at[other])):
            copy = pltpu.make_async_remote_copy(
                src_ref=source,
                dst_ref=held.at[col, row, kind],
                send_sem=plane_send.at[step - 1, kind],
                recv_sem=plane_recv.at[step - 1, kind],
                device_id=device(other * share + lane, col),
                device_id_type=MESH,
            )
            copy.start()
            plane.append(copy)

    def plane_in(piece, kind):
        spot = held.at[col, chip_at(piece) * share + lane, kind]
        return pltpu.make_async_remote_copy(
            src_ref=spot,
            dst_ref=spot,
            send_sem=plane_send.at[piece - 1, kind],
            recv_sem=plane_recv.at[piece - 1, kind],
            device_id=device(chip_at(piece) * share + lane, col),
            device_id_type=MESH,
        )

    def held_here(step, way):
        source = col - way * step
        return jnp.logical_and(source >= 0, source < cols)

    def passes_on(step, way):
        target = col + way
        return jnp.logical_and(held_here(step, way), jnp.logical_and(target >= 0, target < cols))

    def col_copy(step, way, piece, arriving):
        source = col - way * (step + 1) if arriving else col - way * step
        spot = held.at[source, chip_at(piece) * share + lane]
        return pltpu.make_async_remote_copy(
            src_ref=spot,
            dst_ref=spot,
            send_sem=col_send.at[step, ways.index(way), piece],
            recv_sem=col_recv.at[step, ways.index(way), piece],
            device_id=device(row, col - way if arriving else col + way),
            device_id_type=MESH,
        )

    def side_copy(source, piece, other, arriving):
        there = lax.rem(lane - other + share, share) if arriving else lane
        spot = held.at[source, chip_at(piece) * share + there]
        return pltpu.make_async_remote_copy(
            src_ref=spot,
            dst_ref=spot,
            send_sem=side_send.at[source, piece, other - 1],
            recv_sem=side_recv.at[source, piece, other - 1],
            device_id=device(head * share + lax.rem(lane + other, share), col),
            device_id_type=MESH,
        )

    def relay(step, piece):
        for way in ways:
            if step:
                @pl.when(held_here(step, way))
                def _(way=way):
                    col_copy(step - 1, way, piece, True).wait_recv()

            if step < cols - 1:
                @pl.when(passes_on(step, way))
                def _(way=way):
                    col_copy(step, way, piece, False).start()

            if step or way == 1:
                @pl.when(held_here(step, way))
                def _(way=way):
                    for other in range(1, share):
                        side_copy(col - way * step, piece, other, False).start()

    def relay_own(piece):
        if piece:
            plane_in(piece, 0).wait_recv()
            plane_in(piece, 1).wait_recv()
        relay(0, piece)

    relay_own(0)
    loads[4].wait()
    for index in range(rows):
        for member in range(heads):
            part = query_ref[index, :, member * HEAD_DIM : (member + 1) * HEAD_DIM].astype(jnp.float32) * SCALE
            high = part.astype(queries.dtype)
            low = (part - high.astype(jnp.float32)).astype(queries.dtype)
            lines = slice(member * tokens, (member + 1) * tokens)
            queries[index, :HEAD_DIM, lines] = high.T
            queries[index, HEAD_DIM:, lines] = low.T
    across = lax.broadcasted_iota(jnp.int32, (tokens, tokens), 1)
    lower[...] = lax.broadcasted_iota(jnp.int32, (tokens, tokens), 0) - across
    loads[3].wait()

    left, right = col, cols - 1 - col
    both = jnp.minimum(left, right)

    def plane_of(phase):
        near = (phase + 1) // 2
        paired = jnp.where(phase % 2 == 1, col - near, col + near)
        far = phase - both
        single = jnp.where(left > right, col - far, col + far)
        return jnp.where(phase <= 2 * both, paired, single)

    def block_of(turn):
        half = share // 2
        slot, part = turn // half, half - 1 - turn % half
        straight = 1 - jnp.minimum(slot // 4, 1)
        outer = 1 - slot // 6
        along = outer * (1 - straight * (slot % 2))
        down = outer * (1 - straight * (1 - slot % 2))
        shift = jnp.where(slot < 4, slot // 2, jnp.where(slot < 6, slot % 2, 7 - slot))
        chip = lax.rem(head // SIDE + down, SIDE) * SIDE + lax.rem(head % SIDE + along, SIDE)
        return chip * share + lax.rem(lane + shift * half + part, share)

    def parts_of(step):
        source = plane_of(step) if step else col
        return [
            (step, source, [chip_at(piece) * share + 2 * half + one for one in range(2)])
            for piece in range(KVHEADS)
            for half in range(share // 2)
        ]

    def ready(step, start, stop):
        source = plane_of(step) if step else col
        for piece in range(start, stop):
            for other in range(1, share):
                side_copy(source, piece, other, True).wait_recv()

    def produce(part, number, turn, cut, buffer, newest):
        near, source, spans = part
        index = block_of(turn)
        place = order_ref[index * cols + col]
        keys = held[source, pl.ds(spans[0], 2), 0].reshape(block, HEAD_DIM)
        scores = jnp.dot(
            jnp.concatenate([keys, keys], axis=1), queries[index, :, cut], preferred_element_type=jnp.float32
        )
        for half, span in enumerate(spans):
            lines = scores[half * tokens : (half + 1) * tokens]
            if near == 0:
                limit = jnp.where(index == span, 0, tokens)
                shown = jnp.concatenate([lower[...]] * (tile // tokens), axis=1) <= limit
                lines = jnp.where(shown, lines, masked_score)
            spot = (2 * number + half) * tokens
            buffer[spot : spot + tokens, cut] = lines
            top = jnp.max(lines.reshape(tokens // 8, 8, tile), axis=0)
            newest = jnp.maximum(newest, jnp.where(order_ref[span * cols + source] <= place, top, masked_score))
        return newest

    def consume(part, number, turn, cut, buffer, level, summed):
        near, source, spans = part
        place = order_ref[block_of(turn) * cols + col]
        raised, columns = [], []
        for half, span in enumerate(spans):
            ceiling = jnp.where(order_ref[span * cols + source] <= place, level, -masked_score)
            spot = (2 * number + half) * tokens
            raised.append(jnp.exp2(buffer[spot : spot + tokens, cut] - ceiling).astype(held.dtype))
            columns.append(held[source, span, 1])
        ones = jnp.ones((ONES, block), held.dtype)
        weighed = jnp.concatenate([jnp.concatenate(columns, axis=1), ones], axis=0)
        update = jnp.dot(weighed, jnp.concatenate(raised, axis=0), preferred_element_type=jnp.float32)
        return update if summed is None else summed + update

    cuts = [slice(start, start + tile) for start in range(0, width, tile)]

    def first(buffer):
        for cut in cuts:
            newest = jnp.full((8, tile), masked_score, jnp.float32)
            for number, part in enumerate(parts_of(0)):
                newest = produce(part, number, 0, cut, buffer, newest)
            tops[:, cut] = newest

    def unit(step, turn, now, later, following, late=0):
        index = block_of(turn)
        parts = parts_of(step)
        coming = [] if following is None else parts_of(following[0])
        highest = jnp.max(tops[...], axis=0, keepdims=True)
        if step:
            before = best[index, 0:1, :]
            highest = jnp.maximum(before, highest)
            shrink = jnp.exp2(before - highest)
        best[index] = jnp.broadcast_to(highest, (8, width))
        for cut in cuts:
            newest = jnp.full((8, tile), masked_score, jnp.float32)
            summed = None
            for number in range(len(parts)):
                if number < len(coming) - late:
                    newest = produce(coming[number], number, following[1], cut, later, newest)
                summed = consume(parts[number], number, turn, cut, now, highest[:, cut], summed)
            if following is not None:
                tops[:, cut] = newest
            if step:
                summed = total[index, :, cut] * shrink[:, cut] + summed
            if step < cols - 1:
                total[index, :, cut] = summed
            else:
                share_of = summed[:HEAD_DIM] / summed[HEAD_DIM : HEAD_DIM + 1]
                for member in range(tile // tokens):
                    spot = cut.start // tokens * HEAD_DIM + member * HEAD_DIM
                    stage[turn, :, spot : spot + HEAD_DIM] = (
                        share_of[:, member * tokens : (member + 1) * tokens].T.astype(stage.dtype)
                    )

    def rest(step, late, buffer):
        for cut in cuts:
            newest = tops[:, cut]
            for number, part in list(enumerate(parts_of(step)))[-late:]:
                newest = produce(part, number, 0, cut, buffer, newest)
            tops[:, cut] = newest

    def part_copy(turn):
        return pltpu.make_async_remote_copy(
            src_ref=stage.at[turn],
            dst_ref=out_ref.at[:, mine],
            send_sem=part_send.at[turn],
            recv_sem=part_recv.at[turn],
            device_id=device(block_of(turn), col),
            device_id_type=MESH,
        )

    pairs = rows // 2
    last = rows - 1
    hooks = [[(POS[piece] * last // 7, step, piece) for piece in range(KVHEADS)] for step in range(1, cols)]
    hooks += [[]]

    def passing(step, piece):
        if step:
            relay(step, piece)
        else:
            relay_own(piece)

    for piece in range(1,KVHEADS): relay_own(piece)
    ready(0, 0, KVHEADS)
    first(scores_even)
    for step in range(cols):
        final = step == cols - 1

        def pass_at(turn, choices, step=step):
            for when, which, piece in hooks[step]:
                if when in choices:
                    @pl.when(turn == when)
                    def _(which=which, piece=piece):
                        passing(which, piece)

        def body(pair, carry, step=step, final=final, pass_at=pass_at):
            turn = 2 * pair
            pass_at(turn, range(0, last, 2))
            unit(step, turn, scores_even, scores_odd, (step, turn + 1))
            if final:
                part_copy(turn).start()
            pass_at(turn + 1, range(1, last, 2))
            unit(step, turn + 1, scores_odd, scores_even, (step, turn + 2))
            if final:
                part_copy(turn + 1).start()
            return carry

        lax.fori_loop(0, pairs - 1, body, 0)
        turn = last - 1
        pass_at(turn, (turn,))
        unit(step, turn, scores_even, scores_odd, (step, last))
        if final:
            part_copy(turn).start()
            unit(step, last, scores_odd, scores_even, None)
        else:
            pass_at(last, (last,))
            ready(step + 1, 0, KVHEADS - 1)
            unit(step, last, scores_odd, scores_even, (step + 1, 0), share // 2)
            ready(step + 1, KVHEADS - 1, KVHEADS)
            rest(step + 1, share // 2, scores_even)

    own = pltpu.make_async_copy(stage.at[rows - 1], out_ref.at[:, mine], own_sem)
    own.start()
    for copy in plane:
        copy.wait_send()
    for step in range(cols):
        for way in ways:
            if step < cols - 1:
                @pl.when(passes_on(step, way))
                def _(way=way):
                    for piece in range(KVHEADS):
                        col_copy(step, way, piece, False).wait_send()

            if step or way == 1:
                @pl.when(held_here(step, way))
                def _(way=way):
                    for piece in range(KVHEADS):
                        for other in range(1, share):
                            side_copy(col - way * step, piece, other, False).wait_send()
    own.wait()
    for turn in range(rows - 1):
        part_copy(turn).wait()


def fused(query, key, value, span_order, rows, cols):
    tokens = key.shape[0]
    share = rows // KVHEADS
    width = query.shape[2] // rows
    heads = width // HEAD_DIM
    lines = heads * tokens
    kind = query.dtype
    real = jnp.float32
    dma = pltpu.SemaphoreType.DMA
    return pl.pallas_call(
        functools.partial(fused_kernel, rows, cols, heads),
        out_shape=jax.ShapeDtypeStruct((tokens, rows * width), kind),
        in_specs=[pl.BlockSpec(memory_space=pl.ANY)] * 4,
        out_specs=pl.BlockSpec(memory_space=pl.ANY),
        scratch_shapes=[
            pltpu.SMEM(span_order.shape, jnp.int32),
            pltpu.VMEM((rows, tokens, width), kind),
            pltpu.VMEM(key.shape, kind),
            pltpu.VMEM(value.shape, kind),
            pltpu.VMEM((KVHEADS, HEAD_DIM, tokens), kind),
            pltpu.VMEM((cols, rows, 2, tokens, HEAD_DIM), kind),
            pltpu.VMEM((rows, 2 * HEAD_DIM, lines), kind),
            pltpu.VMEM((rows * tokens, lines), real),
            pltpu.VMEM((rows * tokens, lines), real),
            pltpu.VMEM((rows, HEAD_DIM + ONES, lines), real),
            pltpu.VMEM((rows, 8, lines), real),
            pltpu.VMEM((8, lines), real),
            pltpu.VMEM((tokens, tokens), jnp.int32),
            pltpu.VMEM((rows, tokens, width), kind),
            dma((5,)),
            dma((KVHEADS - 1, 2)),
            dma((KVHEADS - 1, 2)),
            dma((cols - 1, 2, KVHEADS)),
            dma((cols - 1, 2, KVHEADS)),
            dma((cols, KVHEADS, share - 1)),
            dma((cols, KVHEADS, share - 1)),
            dma(()),
            dma((rows - 1,)),
            dma((rows - 1,)),
        ],
        compiler_params=pltpu.CompilerParams(
            collective_id=0, has_side_effects=True, vmem_limit_bytes=VMEM_LIMIT
        ),
        name="fused",
    )(*(pltpu.with_memory_space_constraint(array, pltpu.HBM) for array in (span_order, query, key, value)))


def finish_kernel(whole_ref, out_ref, sem):
    copy = pltpu.make_async_copy(whole_ref, out_ref, sem)
    copy.start()
    copy.wait()


def finish(whole):
    return pl.pallas_call(
        finish_kernel,
        out_shape=jax.ShapeDtypeStruct(whole.shape, whole.dtype),
        in_specs=[pl.BlockSpec(memory_space=pltpu.VMEM)],
        out_specs=pl.BlockSpec(memory_space=pl.ANY),
        scratch_shapes=[pltpu.SemaphoreType.DMA(())],
        compiler_params=pltpu.CompilerParams(vmem_limit_bytes=4 * 1024 * 1024),
        name="finish",
    )(whole)


def shards(query, key, value, span_order):
    return finish(fused(query, key, value, span_order, lax.axis_size("row"), lax.axis_size("col")))


def solution(mesh):
    placed = (P(None, "col", None), P(("row", "col"), None), P(("row", "col"), None), P())
    return jax.shard_map(
        shards, mesh=mesh, in_specs=placed, out_specs=P(("row", "col"), None), check_vma=False
    )
```
